32 devices in a mesh: blk: 8 (over z, y), rep: 4 (over x, core).
Axes of the slice: x: 2, y: 2, z: 4, core: 2. Of those that a mesh axis runs over, the one named last changes fastest.
Arguments:
- embeddings: bfloat16 [3072, 1024], P(('blk', 'rep')), may hold values from -60 to 60, as said below
Outputs:
- nearest: float32 [3072, 8], P(('blk', 'rep'))
- dup_count: float32 [3072], P(('blk', 'rep'))
The draws below stay inside these ranges and needn't reach their ends.
Inputs may be any that keep to these rules, and one draw needn't show every extreme that they name: Real-valued embeddings; no row is zero.
All inputs are finite; a program needn't handle non-finite values.
Results may differ from the reference program's by a relative error of at most 0.00068.
Values may be sent and summed in bfloat16 or wider, within the bound.
No kernel may reach another device: no remote copies, remote signals or barrier semaphores. Data moves between devices by JAX's collectives and lax.ppermute only.
A program may use at most 128 MiB of HBM per device.

```python
import math
import jax
import jax.numpy as jnp
from jax import lax

D = 1024
TOPK = 8
NROWS = 3072
NCLUST = 384
N_BLK = 8


def draw_embeddings(key, part):
    keys = jax.random.split(key, 5)
    labels = jax.random.randint(keys[0], (NROWS,), 0, NCLUST)
    centers = jax.random.normal(keys[1], (NCLUST, D), jnp.float32)
    noise = jax.random.normal(keys[2], (NROWS, D), jnp.float32)
    blend_factor = jax.random.uniform(keys[3], (NROWS, 1), jnp.float32, 0.3, 0.95)
    scales = jnp.exp(jax.random.uniform(keys[4], (NROWS, 1), jnp.float32, 0.0, math.log(10.0)))
    rows = blend_factor * centers[labels] + jnp.sqrt(1.0 - blend_factor * blend_factor) * noise
    return jnp.clip(rows * scales, -60.0, 60.0).astype(jnp.bfloat16)


def setup_inputs(seed: int = 0) -> dict:
    seeds = jax.random.split(jax.random.key(seed), 2)
    embeddings = draw_embeddings(jax.random.fold_in(seeds[1], 71), 0)
    return {"embeddings": embeddings}


decision_bound = 0.5
sigmoid_sharpness = 0.05

def reference(embeddings):
    whole = embeddings.astype(jnp.float32)
    unit = (whole / jnp.sqrt(lax.optimization_barrier(jnp.sum(whole * whole, axis=1, keepdims=True)) + 1e-06)).astype(jnp.bfloat16)
    block_rows = NROWS // N_BLK
    all_ids = jnp.arange(NROWS, dtype=jnp.int32)

    def single_tile(index):
        queries = lax.dynamic_slice_in_dim(unit, index * block_rows, block_rows, 0)
        query_ids = index * block_rows + jnp.arange(block_rows, dtype=jnp.int32)
        cosine_table = jnp.dot(queries, unit.T, preferred_element_type=jnp.float32)
        cosine_table = jnp.where(query_ids[:, None] == all_ids[None, :], -2.0, cosine_table)
        best = lax.top_k(cosine_table, TOPK)[0]
        duplicate_tally = lax.optimization_barrier(jnp.sum(jax.nn.sigmoid((cosine_table - decision_bound) / sigmoid_sharpness), axis=1))
        return (best, duplicate_tally)
    best, duplicate_tally = lax.map(single_tile, jnp.arange(N_BLK, dtype=jnp.int32))
    return (best.reshape(NROWS, TOPK), duplicate_tally.reshape(NROWS))
```

```python
import functools

import jax
import jax.numpy as jnp
from jax import lax
from jax.experimental import pallas as pl
from jax.experimental.pallas import tpu as pltpu
from jax.sharding import PartitionSpec as P

TOPK = 8
SUB = 8
PACK = 16
LOW = -4.0
decision_bound = 0.5
sigmoid_sharpness = 0.05
GRANT = 32 * 2**20
AXES = ("blk", "rep")


SORT8 = (
    (0, 1), (2, 3), (4, 5), (6, 7),
    (0, 2), (1, 3), (4, 6), (5, 7),
    (1, 2), (5, 6), (0, 4), (3, 7),
    (1, 5), (2, 6),
    (1, 4), (3, 6),
    (2, 4), (3, 5),
    (3, 4),
)
BITONIC8 = (
    (0, 4), (1, 5), (2, 6), (3, 7),
    (0, 2), (1, 3), (4, 6), (5, 7),
    (0, 1), (2, 3), (4, 5), (6, 7),
)


def network(values, pairs):
    values = list(values)
    for low, high in pairs:
        a, b = values[low], values[high]
        values[low], values[high] = jnp.maximum(a, b), jnp.minimum(a, b)
    return values


def merge(a, b):
    return network([jnp.maximum(a[i], b[TOPK - 1 - i]) for i in range(TOPK)], BITONIC8)


def soft(table):
    return 1.0 / (1.0 + jnp.exp((decision_bound - table) / sigmoid_sharpness))


def column_lists(table):
    tiles = [table[i : i + SUB] for i in range(0, table.shape[0], SUB)]
    best = None
    for i in range(0, len(tiles), TOPK):
        group = tiles[i : i + TOPK]
        group += [jnp.full_like(tiles[0], LOW)] * (TOPK - len(group))
        group = network(group, SORT8)
        best = group if best is None else merge(best, group)
    count = functools.reduce(jnp.add, [soft(t) for t in tiles])
    return best, count


def fold_sublanes(best, count):
    for step in (4, 2, 1):
        best = merge(best, [pltpu.roll(b, step, 0) for b in best])
        count = count + pltpu.roll(count, step, 0)
    place = lax.broadcasted_iota(jnp.int32, best[0].shape, 0)
    top = best[0]
    for i in range(1, TOPK):
        top = jnp.where(place == i, best[i], top)
    return top, count


def dots(a, b):
    return lax.dot_general(a, b, (((1,), (1,)), ((), ())), preferred_element_type=jnp.float32)


def unit_kernel(x_ref, o_ref):
    whole = x_ref[...].astype(jnp.float32)
    length = jnp.sqrt(jnp.sum(whole * whole, axis=1, keepdims=True) + 1e-06)
    o_ref[...] = (whole / length).astype(jnp.bfloat16)


def score_kernel(n_query, n_shift, here, *refs):
    mine = refs[:n_query]
    theirs = refs[n_query : 2 * n_query]
    shifted = refs[2 * n_query : 2 * n_query + 2 * n_shift]
    sent = refs[2 * n_query + 2 * n_shift : 3 * n_query + 2 * n_shift]
    keyed = refs[3 * n_query + 2 * n_shift :]
    rows = mine[0].shape[0]
    live = here()
    query = jnp.concatenate([q[...] for q in mine], axis=0)
    other = jnp.concatenate([q[...] for q in theirs], axis=0)
    table = dots(mine[0][...], query)
    line = lax.broadcasted_iota(jnp.int32, table.shape, 0)
    column = lax.broadcasted_iota(jnp.int32, table.shape, 1)
    table = jnp.where(line == column, -2.0, table)
    best, count = column_lists(jnp.concatenate([table, dots(theirs[0][...], query)], axis=0))
    for k in range(n_shift):
        key, twin = shifted[2 * k][...], shifted[2 * k + 1][...]
        more, more_count = column_lists(
            jnp.concatenate([dots(key, query), dots(twin, query)], axis=0)
        )
        if live[k] is not None:
            more = [jnp.where(live[k], m, LOW) for m in more]
            more_count = jnp.where(live[k], more_count, 0.0)
        best = merge(best, more)
        count = count + more_count
        store(
            keyed[k],
            *fold_sublanes(
                *column_lists(jnp.concatenate([dots(query, key), dots(other, key)], axis=0))
            ),
        )
    top, total = fold_sublanes(best, count)
    for j in range(n_query):
        store(sent[j], top[:, j * rows : (j + 1) * rows], total[:, j * rows : (j + 1) * rows])


def store(ref, top, total):
    ref[:SUB] = top
    ref[SUB:] = total


def lists_of(ref):
    shape = (SUB, ref.shape[1])
    row = lambda i: jnp.broadcast_to(ref[i : i + 1], shape)
    return [row(i) for i in range(TOPK)], ref[SUB:]


def last_kernel(n_query, n_shift, here, *refs):
    parts = refs[: n_query + n_shift]
    near_ref, dup_ref = refs[n_query + n_shift :]
    live = [None] * n_query + here()
    found = []
    for flag, part in zip(live, parts):
        best, count = lists_of(part)
        if flag is not None:
            best = [jnp.where(flag, b, LOW) for b in best]
            count = jnp.where(flag, count, 0.0)
        found.append((best, count))
    while len(found) > 1:
        paired = [
            (merge(found[i][0], found[i + 1][0]), found[i][1] + found[i + 1][1])
            for i in range(0, len(found) - 1, 2)
        ]
        found = paired + found[len(found) - len(found) % 2 :]
    best, count = found[0]
    for i in range(TOPK):
        near_ref[i : i + 1] = best[i][:1]
    dup_ref[...] = count[:1]


VMEM = pl.BlockSpec(memory_space=pltpu.VMEM)


def call(kernel, args, shapes, keep=True):
    args = [pltpu.with_memory_space_constraint(a, pltpu.VMEM) for a in args]
    return pl.pallas_call(
        kernel,
        out_shape=[(pltpu.VMEM if keep else jax.ShapeDtypeStruct)(*s) for s in shapes],
        in_specs=[VMEM] * len(args),
        out_specs=[VMEM] * len(shapes),
        compiler_params=pltpu.CompilerParams(vmem_limit_bytes=GRANT),
    )(*args)


def body(blocks, reps, embeddings):
    rows = embeddings.shape[0]
    cores = 2 if reps % 2 == 0 else 1
    wide = reps // cores
    high = 2 if blocks % 2 == 0 else 1
    deep = blocks // high

    def flat(z, y, x, c):
        return ((z * high + y) * wide + x) * cores + c

    places = [
        (z, y, x, c)
        for z in range(deep)
        for y in range(high)
        for x in range(wide)
        for c in range(cores)
    ]

    def moved(value, to):
        perm = [(flat(*p), flat(*to(*p))) for p in places if to(*p) is not None]
        return lax.ppermute(value, AXES, perm)

    def back(value, to):
        perm = [(flat(*to(*p)), flat(*p)) for p in places if to(*p) is not None]
        return lax.ppermute(value, AXES, perm)

    plane = [
        (lambda z, y, x, c, dy=dy, dx=dx: (z, (y + dy) % high, (x + dx) % wide, c))
        for dy in range(high)
        for dx in range(wide)
        if dy or dx
    ]
    half = deep // 2

    def shift(k):
        def to(z, y, x, c):
            if 2 * k == deep:
                if z < half:
                    return (z + half, y, x, c) if z % 2 == 0 else None
                return (z - half, y, x, c) if (z - half) % 2 == 1 else None
            return ((z + k) % deep, y, x, c)

        return to

    shifts = [shift(k) for k in range(1, half + 1)]
    swap = lambda z, y, x, c: (z, y, x, (c + 1) % cores)

    def sends(k):
        if 2 * k != deep:
            return None
        depth = lax.axis_index("blk") // high
        return jnp.where(depth < half, depth % 2 == 0, (depth - half) % 2 == 1)

    def gave():
        return [sends(k) for k in range(1, half + 1)]

    def got():
        return [None if g is None else jnp.logical_not(g) for g in gave()]

    unit = pl.pallas_call(
        unit_kernel,
        out_shape=pltpu.VMEM(embeddings.shape, jnp.bfloat16),
        in_specs=[VMEM],
        out_specs=VMEM,
        compiler_params=pltpu.CompilerParams(vmem_limit_bytes=GRANT),
    )(embeddings)
    far = [moved(unit, to) for to in shifts]
    near = [unit] + [moved(unit, to) for to in plane]
    twins = [moved(n, swap) for n in near]
    keys = []
    for f in far:
        keys += [f, moved(f, swap)]

    n_query, n_shift = len(near), len(far)
    packed = ((PACK, rows), jnp.float32)
    out = call(
        functools.partial(score_kernel, n_query, n_shift, got),
        near + twins + keys,
        [packed] * (n_query + n_shift),
    )
    home = [out[0]]
    home += [back(out[1 + j], to) for j, to in enumerate(plane)]
    home += [back(out[n_query + k], to) for k, to in enumerate(shifts)]
    near8, dup = call(
        functools.partial(last_kernel, n_query, n_shift, gave),
        home,
        [((TOPK, rows), jnp.float32), ((1, rows), jnp.float32)],
        keep=False,
    )
    return near8.T, dup.reshape(rows)


def solution(mesh):
    placed = (P(AXES, None),)
    return jax.shard_map(
        functools.partial(body, mesh.shape["blk"], mesh.shape["rep"]),
        mesh=mesh,
        in_specs=placed,
        out_specs=(P(AXES, None), P(AXES)),
        check_vma=False,
    )
```

```python
import functools

import jax
import jax.numpy as jnp
from jax import lax
from jax.experimental import pallas as pl
from jax.experimental.pallas import tpu as pltpu
from jax.sharding import PartitionSpec as P


TOPK = 8
SUB = 8
PACK = 16
LOW = -4.0
decision_bound = 0.5
sigmoid_sharpness = 0.05
GRANT = 32 * 2**20
AXES = ("blk", "rep")


SORT8 = (
    (0, 1), (2, 3), (4, 5), (6, 7),
    (0, 2), (1, 3), (4, 6), (5, 7),
    (1, 2), (5, 6), (0, 4), (3, 7),
    (1, 5), (2, 6),
    (1, 4), (3, 6),
    (2, 4), (3, 5),
    (3, 4),
)
BITONIC8 = (
    (0, 4), (1, 5), (2, 6), (3, 7),
    (0, 2), (1, 3), (4, 6), (5, 7),
    (0, 1), (2, 3), (4, 5), (6, 7),
)


def network(values, pairs):
    values = list(values)
    for low, high in pairs:
        a, b = values[low], values[high]
        values[low], values[high] = jnp.maximum(a, b), jnp.minimum(a, b)
    return values


def merge(a, b):
    return network([jnp.maximum(a[i], b[TOPK - 1 - i]) for i in range(TOPK)], BITONIC8)


def soft(table):
    return 1.0 / (1.0 + jnp.exp((decision_bound - table) / sigmoid_sharpness))


def column_lists(table):
    tiles = [table[i : i + SUB] for i in range(0, table.shape[0], SUB)]
    best = None
    for i in range(0, len(tiles), TOPK):
        group = tiles[i : i + TOPK]
        group += [jnp.full_like(tiles[0], LOW)] * (TOPK - len(group))
        group = network(group, SORT8)
        best = group if best is None else merge(best, group)
    count = functools.reduce(jnp.add, [soft(t) for t in tiles])
    return best, count


def fold_sublanes(best, count):
    for step in (4, 2, 1):
        best = merge(best, [pltpu.roll(b, step, 0) for b in best])
        count = count + pltpu.roll(count, step, 0)
    place = lax.broadcasted_iota(jnp.int32, best[0].shape, 0)
    top = best[0]
    for i in range(1, TOPK):
        top = jnp.where(place == i, best[i], top)
    return top, count


def dots(a, b):
    return lax.dot_general(a, b, (((1,), (1,)), ((), ())), preferred_element_type=jnp.float32)


def unit_rows(block):
    whole = block.astype(jnp.float32)
    length = jnp.sqrt(jnp.sum(whole * whole, axis=1, keepdims=True) + 1e-06)
    return (whole / length).astype(jnp.bfloat16)


def unit_kernel(x_ref, o_ref):
    o_ref[...] = unit_rows(x_ref[...])


def store(ref, top, total, start=0):
    columns = pl.ds(start, top.shape[1])
    ref[:SUB, columns] = top
    ref[SUB:, columns] = total


def join_kernel(a_ref, b_ref, o_ref):
    rows = a_ref.shape[0]
    o_ref[:rows] = a_ref[...]
    o_ref[rows:] = unit_rows(b_ref[...])


def split_queries(pair, direct, relayed, corner, corner_twin):
    rows = corner.shape[0]
    keep = jnp.concatenate([pair[:rows], direct[...], corner[...]], axis=0)
    give = jnp.concatenate([pair[rows:], relayed[...], corner_twin[...]], axis=0)
    return keep, give


def home_kernel(pair, direct, relayed, corner, corner_twin, keep_ref, give_ref):
    rows = corner.shape[0]
    own = pair[:rows]
    for own_first, query, ref in zip(
        (True, False), split_queries(pair, direct, relayed, corner, corner_twin), (keep_ref, give_ref)
    ):
        table = dots(own, query)
        if own_first:
            line = lax.broadcasted_iota(jnp.int32, table.shape, 0)
            column = lax.broadcasted_iota(jnp.int32, table.shape, 1)
            table = jnp.where(line == column, -2.0, table)
        best, count = column_lists(table)
        for i in range(TOPK):
            ref[i * SUB : (i + 1) * SUB] = best[i]
        ref[TOPK * SUB :] = count


def score_kernel(n_shift, got, *refs):
    queries, states = refs[:5], refs[5:7]
    keys = refs[7 : 7 + n_shift]
    keep_ref, give_ref = refs[7 + n_shift : 9 + n_shift]
    back_refs = refs[9 + n_shift :]
    live = got()
    keep, give = split_queries(*queries)
    for query, state, ref in ((keep, states[0], keep_ref), (give, states[1], give_ref)):
        best = [state[i * SUB : (i + 1) * SUB] for i in range(TOPK)]
        count = state[TOPK * SUB :]
        for k in range(n_shift):
            more, more_count = column_lists(dots(keys[k][...], query))
            best = merge(best, [jnp.where(live[k], m, LOW) for m in more])
            count = count + jnp.where(live[k], more_count, 0.0)
        store(ref, *fold_sublanes(best, count))
    for k in range(n_shift):
        key = keys[k][...]
        table = jnp.concatenate([dots(keep, key), dots(give, key)], axis=0)
        store(back_refs[k], *fold_sublanes(*column_lists(table)))


def lists_of(packed):
    shape = (SUB, packed.shape[1])
    row = lambda i: jnp.broadcast_to(packed[i : i + 1], shape)
    return [row(i) for i in range(TOPK)], packed[SUB:]


def stacked(best):
    place = lax.broadcasted_iota(jnp.int32, best[0].shape, 0)
    top = best[0]
    for i in range(1, TOPK):
        top = jnp.where(place == i, best[i], top)
    return top


def pair_kernel(keep_ref, got_ref, own_ref, direct_ref, corner_ref):
    rows = own_ref.shape[1]
    best, count = lists_of(keep_ref[...])
    more, more_count = lists_of(got_ref[...])
    top, total = stacked(merge(best, more)), count + more_count
    store(own_ref, top[:, :rows], total[:, :rows])
    store(direct_ref, top[:, rows : 3 * rows], total[:, rows : 3 * rows])
    store(corner_ref, top[:, 3 * rows :], total[:, 3 * rows :])


def last_kernel(n_shift, gave, own, corner, direct, relayed, *refs):
    mine, theirs = refs[:n_shift], refs[n_shift : 2 * n_shift]
    near_ref, dup_ref = refs[2 * n_shift :]
    rows = own.shape[1]
    found = [lists_of(own[...]), lists_of(corner[...])]
    found += [lists_of(direct[:, :rows]), lists_of(relayed[:, rows:])]
    parts = [m[:, :rows] for m in mine] + [t[:, rows:] for t in theirs]
    for flag, part in zip(gave(False) + gave(True), parts):
        best, count = lists_of(part)
        found.append(([jnp.where(flag, b, LOW) for b in best], jnp.where(flag, count, 0.0)))
    while len(found) > 1:
        paired = [
            (merge(found[i][0], found[i + 1][0]), found[i][1] + found[i + 1][1])
            for i in range(0, len(found) - 1, 2)
        ]
        found = paired + found[len(found) - len(found) % 2 :]
    best, count = found[0]
    near_ref[...] = stacked(best)
    dup_ref[...] = count[:1]


VMEM = pl.BlockSpec(memory_space=pltpu.VMEM)


def call(kernel, args, shapes, keep=True):
    args = [pltpu.with_memory_space_constraint(a, pltpu.VMEM) for a in args]
    return pl.pallas_call(
        kernel,
        out_shape=[(pltpu.VMEM if keep else jax.ShapeDtypeStruct)(*s) for s in shapes],
        in_specs=[VMEM] * len(args),
        out_specs=[VMEM] * len(shapes),
        compiler_params=pltpu.CompilerParams(vmem_limit_bytes=GRANT),
    )(*args)


def body(blocks, reps, embeddings):
    rows, width = embeddings.shape
    deep, wide = blocks // 2, reps // 2
    half = deep // 2
    n_shift = (half + 1) // 2
    f32, bf16 = jnp.float32, jnp.bfloat16

    def flat(z, y, x, c):
        return ((z * 2 + y) * wide + x) * 2 + c

    places = [
        (z, y, x, c) for z in range(deep) for y in range(2) for x in range(wide) for c in range(2)
    ]

    def moved(value, to, reverse=False):
        perm = [(flat(*p), flat(*to(*p))) for p in places if to(*p) is not None]
        return lax.ppermute(value, AXES, [(b, a) for a, b in perm] if reverse else perm)

    def swap(z, y, x, c):
        return z, y, x, 1 - c

    def side(z, y, x, c):
        return (z, y, (x + 1) % wide, c) if c == 0 else (z, 1 - y, x, c)

    def corner(z, y, x, c):
        return z, 1 - y, (x + 1) % wide, c

    def shift(j):
        def to(z, y, x, c):
            k = 2 * j + 1 + c
            if k > half:
                return None
            if 2 * k == deep:
                if z < half:
                    return (z + half, y, x, c) if z % 2 == 0 else None
                return (z - half, y, x, c) if (z - half) % 2 == 1 else None
            return (z + k) % deep, y, x, c

        return to

    def flags(other, pick):
        depth = lax.axis_index("blk") // 2
        core = lax.axis_index("rep") % 2
        core = 1 - core if other else core
        sends = jnp.where(depth < half, depth % 2 == 0, (depth - half) % 2 == 1)
        out = []
        for j in range(n_shift):
            k = 2 * j + 1 + core
            whole = 2 * k != deep
            out.append((k <= half) & (whole | (sends == pick)))
        return out

    def gave(other):
        return flags(other, True)

    def got():
        return flags(False, False)

    twin = moved(embeddings, swap)
    unit = pl.pallas_call(
        unit_kernel,
        out_shape=pltpu.VMEM(embeddings.shape, bf16),
        in_specs=[VMEM],
        out_specs=VMEM,
        compiler_params=pltpu.CompilerParams(vmem_limit_bytes=GRANT),
    )(embeddings)
    corner_rows = moved(unit, corner)
    (pair,) = call(join_kernel, [unit, twin], [((2 * rows, width), bf16)])
    keys = [moved(pair, shift(j)) for j in range(n_shift)]
    direct = moved(pair, side)
    corner_twin = moved(corner_rows, swap)
    relayed = moved(direct, swap)
    queries = [pair, direct, relayed, corner_rows, corner_twin]

    state = (((TOPK + 1) * SUB, 4 * rows), f32)
    states = call(home_kernel, queries, [state, state])
    lists = lambda n: ((PACK, n * rows), f32)
    keep, give, *away = call(
        functools.partial(score_kernel, n_shift, got),
        queries + list(states) + keys,
        [lists(4), lists(4)] + [lists(2)] * n_shift,
    )
    given = moved(give, swap)
    mine = [moved(a, shift(j), reverse=True) for j, a in enumerate(away)]
    own, sides, corners = call(pair_kernel, [keep, given], [lists(1), lists(2), lists(1)])
    direct = moved(sides, side, reverse=True)
    corners = moved(corners, corner, reverse=True)
    theirs = [moved(m, swap) for m in mine]
    relayed = moved(direct, swap)
    near, dup = call(
        functools.partial(last_kernel, n_shift, gave),
        [own, corners, direct, relayed] + mine + theirs,
        [((TOPK, rows), f32), ((1, rows), f32)],
        keep=False,
    )
    return near.T, dup.reshape(rows)


def solution(mesh):
    placed = (P(AXES, None),)

    def layer(embeddings):
        return body(mesh.shape["blk"], mesh.shape["rep"], embeddings)

    return jax.shard_map(
        layer,
        mesh=mesh,
        in_specs=placed,
        out_specs=(P(AXES, None), P(AXES)),
        check_vma=False,
    )
```

```python
import functools

import jax
import jax.numpy as jnp
from jax import lax
from jax.experimental import pallas as pl
from jax.experimental.pallas import tpu as pltpu
from jax.sharding import PartitionSpec as P


TOPK = 8
SUB = 8
PACK = 16
LOW = -4.0
decision_bound = 0.5
sigmoid_sharpness = 0.05
GRANT = 32 * 2**20
AXES = ("blk", "rep")


SORT8 = (
    (0, 1), (2, 3), (4, 5), (6, 7),
    (0, 2), (1, 3), (4, 6), (5, 7),
    (1, 2), (5, 6), (0, 4), (3, 7),
    (1, 5), (2, 6),
    (1, 4), (3, 6),
    (2, 4), (3, 5),
    (3, 4),
)
BITONIC8 = (
    (0, 4), (1, 5), (2, 6), (3, 7),
    (0, 2), (1, 3), (4, 6), (5, 7),
    (0, 1), (2, 3), (4, 5), (6, 7),
)


def network(values, pairs):
    values = list(values)
    for low, high in pairs:
        a, b = values[low], values[high]
        values[low], values[high] = jnp.maximum(a, b), jnp.minimum(a, b)
    return values


def merge(a, b):
    return network([jnp.maximum(a[i], b[TOPK - 1 - i]) for i in range(TOPK)], BITONIC8)


def soft(table):
    return 1.0 / (1.0 + jnp.exp((decision_bound - table) / sigmoid_sharpness))


def column_lists(table):
    tiles = [table[i : i + SUB] for i in range(0, table.shape[0], SUB)]
    best = None
    for i in range(0, len(tiles), TOPK):
        group = tiles[i : i + TOPK]
        group += [jnp.full_like(tiles[0], LOW)] * (TOPK - len(group))
        group = network(group, SORT8)
        best = group if best is None else merge(best, group)
    count = functools.reduce(jnp.add, [soft(t) for t in tiles])
    return best, count


def fold_sublanes(best, count):
    for step in (4, 2, 1):
        best = merge(best, [pltpu.roll(b, step, 0) for b in best])
        count = count + pltpu.roll(count, step, 0)
    place = lax.broadcasted_iota(jnp.int32, best[0].shape, 0)
    top = best[0]
    for i in range(1, TOPK):
        top = jnp.where(place == i, best[i], top)
    return top, count


def dots(a, b):
    return lax.dot_general(a, b, (((1,), (1,)), ((), ())), preferred_element_type=jnp.float32)


def unit_rows(block):
    whole = block.astype(jnp.float32)
    length = jnp.sqrt(jnp.sum(whole * whole, axis=1, keepdims=True) + 1e-06)
    return (whole / length).astype(jnp.bfloat16)


def unit_kernel(x_ref, o_ref):
    o_ref[...] = unit_rows(x_ref[...])


def join_kernel(a_ref, b_ref, o_ref):
    rows = a_ref.shape[0]
    o_ref[:rows] = unit_rows(a_ref[...])
    o_ref[rows:] = unit_rows(b_ref[...])


def store(ref, top, total, start=0):
    columns = pl.ds(start, top.shape[1])
    ref[:SUB, columns] = top
    ref[SUB:, columns] = total


def split_queries(pair, direct, relayed, corner, corner_twin):
    rows = corner.shape[0]
    keep = jnp.concatenate([pair[:rows], direct[...], corner[...]], axis=0)
    give = jnp.concatenate([pair[rows:], relayed[...], corner_twin[...]], axis=0)
    return keep, give


def home_kernel(pair, direct, relayed, corner, corner_twin, keep_ref, give_ref):
    rows = corner.shape[0]
    own = pair[:rows]
    for own_first, query, ref in zip(
        (True, False), split_queries(pair, direct, relayed, corner, corner_twin), (keep_ref, give_ref)
    ):
        table = dots(own, query)
        if own_first:
            line = lax.broadcasted_iota(jnp.int32, table.shape, 0)
            column = lax.broadcasted_iota(jnp.int32, table.shape, 1)
            table = jnp.where(line == column, -2.0, table)
        best, count = column_lists(table)
        for i in range(TOPK):
            ref[i * SUB : (i + 1) * SUB] = best[i]
        ref[TOPK * SUB :] = count


def score_kernel(n_shift, got, *refs):
    queries, states = refs[:5], refs[5:7]
    keys = refs[7 : 7 + n_shift]
    keep_ref, give_ref = refs[7 + n_shift : 9 + n_shift]
    back_refs = refs[9 + n_shift :]
    live = got()
    keep, give = split_queries(*queries)
    for query, state, ref in ((keep, states[0], keep_ref), (give, states[1], give_ref)):
        best = [state[i * SUB : (i + 1) * SUB] for i in range(TOPK)]
        count = state[TOPK * SUB :]
        for k in range(n_shift):
            more, more_count = column_lists(dots(keys[k][...], query))
            best = merge(best, [jnp.where(live[k], m, LOW) for m in more])
            count = count + jnp.where(live[k], more_count, 0.0)
        store(ref, *fold_sublanes(best, count))
    for k in range(n_shift):
        key = keys[k][...]
        table = jnp.concatenate([dots(keep, key), dots(give, key)], axis=0)
        store(back_refs[k], *fold_sublanes(*column_lists(table)))


def lists_of(packed):
    shape = (SUB, packed.shape[1])
    row = lambda i: jnp.broadcast_to(packed[i : i + 1], shape)
    return [row(i) for i in range(TOPK)], packed[SUB:]


def stacked(best):
    place = lax.broadcasted_iota(jnp.int32, best[0].shape, 0)
    top = best[0]
    for i in range(1, TOPK):
        top = jnp.where(place == i, best[i], top)
    return top


def pair_kernel(keep_ref, got_ref, own_ref, direct_ref, corner_ref):
    rows = own_ref.shape[1]
    best, count = lists_of(keep_ref[...])
    more, more_count = lists_of(got_ref[...])
    top, total = stacked(merge(best, more)), count + more_count
    store(own_ref, top[:, :rows], total[:, :rows])
    store(direct_ref, top[:, rows : 3 * rows], total[:, rows : 3 * rows])
    store(corner_ref, top[:, 3 * rows :], total[:, 3 * rows :])


def last_kernel(n_shift, gave, own, corner, direct, relayed, *refs):
    mine, theirs = refs[:n_shift], refs[n_shift : 2 * n_shift]
    near_ref, dup_ref = refs[2 * n_shift :]
    rows = own.shape[1]
    found = [lists_of(own[...]), lists_of(corner[...])]
    found += [lists_of(direct[:, :rows]), lists_of(relayed[:, rows:])]
    parts = [m[:, :rows] for m in mine] + [t[:, rows:] for t in theirs]
    for flag, part in zip(gave(False) + gave(True), parts):
        best, count = lists_of(part)
        found.append(([jnp.where(flag, b, LOW) for b in best], jnp.where(flag, count, 0.0)))
    while len(found) > 1:
        paired = [
            (merge(found[i][0], found[i + 1][0]), found[i][1] + found[i + 1][1])
            for i in range(0, len(found) - 1, 2)
        ]
        found = paired + found[len(found) - len(found) % 2 :]
    best, count = found[0]
    near_ref[...] = stacked(best)
    dup_ref[...] = count[:1]


VMEM = pl.BlockSpec(memory_space=pltpu.VMEM)


def call(kernel, args, shapes, keep=True):
    args = [pltpu.with_memory_space_constraint(a, pltpu.VMEM) for a in args]
    return pl.pallas_call(
        kernel,
        out_shape=[(pltpu.VMEM if keep else jax.ShapeDtypeStruct)(*s) for s in shapes],
        in_specs=[VMEM] * len(args),
        out_specs=[VMEM] * len(shapes),
        compiler_params=pltpu.CompilerParams(vmem_limit_bytes=GRANT),
    )(*args)


def body(blocks, reps, embeddings):
    rows, width = embeddings.shape
    deep, wide = blocks // 2, reps // 2
    half = deep // 2
    n_shift = (half + 1) // 2
    f32, bf16 = jnp.float32, jnp.bfloat16

    def flat(z, y, x, c):
        return ((z * 2 + y) * wide + x) * 2 + c

    places = [
        (z, y, x, c) for z in range(deep) for y in range(2) for x in range(wide) for c in range(2)
    ]

    def moved(value, to, reverse=False):
        perm = [(flat(*p), flat(*to(*p))) for p in places if to(*p) is not None]
        return lax.ppermute(value, AXES, [(b, a) for a, b in perm] if reverse else perm)

    def swap(z, y, x, c):
        return z, y, x, 1 - c

    def side(z, y, x, c):
        return (z, y, (x + 1) % wide, c) if c == 0 else (z, 1 - y, x, c)

    def corner(z, y, x, c):
        return z, 1 - y, (x + 1) % wide, c

    def shift(j):
        def to(z, y, x, c):
            k = 2 * j + 2 - c
            if k > half:
                return None
            if 2 * k == deep:
                if z < half:
                    return (z + half, y, x, c) if z % 2 == 0 else None
                return (z - half, y, x, c) if (z - half) % 2 == 1 else None
            return (z + k) % deep, y, x, c

        return to

    def flags(other, pick):
        depth = lax.axis_index("blk") // 2
        core = lax.axis_index("rep") % 2
        core = 1 - core if other else core
        sends = jnp.where(depth < half, depth % 2 == 0, (depth - half) % 2 == 1)
        out = []
        for j in range(n_shift):
            k = 2 * j + 2 - core
            whole = 2 * k != deep
            out.append((k <= half) & (whole | (sends == pick)))
        return out

    def gave(other):
        return flags(other, True)

    def got():
        return flags(False, False)

    twin = moved(embeddings, swap)
    corner_rows = moved(embeddings, corner)
    (pair,) = call(join_kernel, [embeddings, twin], [((2 * rows, width), bf16)])
    keys = [moved(pair, shift(j)) for j in range(n_shift)]
    direct = moved(pair, side)
    (corner_rows,) = call(unit_kernel, [corner_rows], [((rows, width), bf16)])
    corner_twin = moved(corner_rows, swap)
    relayed = moved(direct, swap)
    queries = [pair, direct, relayed, corner_rows, corner_twin]

    state = (((TOPK + 1) * SUB, 4 * rows), f32)
    states = call(home_kernel, queries, [state, state])
    lists = lambda n: ((PACK, n * rows), f32)
    keep, give, *away = call(
        functools.partial(score_kernel, n_shift, got),
        queries + list(states) + keys,
        [lists(4), lists(4)] + [lists(2)] * n_shift,
    )
    given = moved(give, swap)
    mine = [moved(a, shift(j), reverse=True) for j, a in enumerate(away)]
    own, sides, corners = call(pair_kernel, [keep, given], [lists(1), lists(2), lists(1)])
    direct = moved(sides, side, reverse=True)
    corners = moved(corners, corner, reverse=True)
    theirs = [moved(m, swap) for m in mine]
    relayed = moved(direct, swap)
    near, dup = call(
        functools.partial(last_kernel, n_shift, gave),
        [own, corners, direct, relayed] + mine + theirs,
        [((TOPK, rows), f32), ((1, rows), f32)],
        keep=False,
    )
    return near.T, dup.reshape(rows)


def solution(mesh):
    placed = (P(AXES, None),)

    def layer(embeddings):
        return body(mesh.shape["blk"], mesh.shape["rep"], embeddings)

    return jax.shard_map(
        layer,
        mesh=mesh,
        in_specs=placed,
        out_specs=(P(AXES, None), P(AXES)),
        check_vma=False,
    )
```

```python
import functools
import math

import jax
import jax.numpy as jnp
from jax import lax
from jax.experimental import pallas as pl
from jax.experimental.pallas import tpu as pltpu
from jax.sharding import PartitionSpec as P


TOPK = 8
SUB = 8
PACK = 16
LOW = -4.0
decision_bound = 0.5
sigmoid_sharpness = 0.05
GRANT = 32 * 2**20
AXES = ("blk", "rep")

SOFT_SLOPE = 1.0 / (sigmoid_sharpness * math.log(2.0))
SOFT_BASE = decision_bound * SOFT_SLOPE


SORT8 = (
    (0, 1), (2, 3), (4, 5), (6, 7),
    (0, 2), (1, 3), (4, 6), (5, 7),
    (1, 2), (5, 6), (0, 4), (3, 7),
    (1, 5), (2, 6),
    (1, 4), (3, 6),
    (2, 4), (3, 5),
    (3, 4),
)
BITONIC8 = (
    (0, 4), (1, 5), (2, 6), (3, 7),
    (0, 2), (1, 3), (4, 6), (5, 7),
    (0, 1), (2, 3), (4, 5), (6, 7),
)


def network(values, pairs):
    values = list(values)
    for low, high in pairs:
        a, b = values[low], values[high]
        values[low], values[high] = jnp.maximum(a, b), jnp.minimum(a, b)
    return values


def merge(a, b):
    return network([jnp.maximum(a[i], b[TOPK - 1 - i]) for i in range(TOPK)], BITONIC8)


def soft(table):
    return 1.0 / (1.0 + jnp.exp2(SOFT_BASE - SOFT_SLOPE * table))


def column_lists(table):
    tiles = [table[i : i + SUB] for i in range(0, table.shape[0], SUB)]
    best = None
    for i in range(0, len(tiles), TOPK):
        group = tiles[i : i + TOPK]
        group += [jnp.full_like(tiles[0], LOW)] * (TOPK - len(group))
        group = network(group, SORT8)
        best = group if best is None else merge(best, group)
    count = functools.reduce(jnp.add, [soft(t) for t in tiles])
    return best, count


def fold_sublanes(best, count):
    for step in (4, 2, 1):
        best = merge(best, [pltpu.roll(b, step, 0) for b in best])
        count = count + pltpu.roll(count, step, 0)
    place = lax.broadcasted_iota(jnp.int32, best[0].shape, 0)
    top = best[0]
    for i in range(1, TOPK):
        top = jnp.where(place == i, best[i], top)
    return top, count


def dots(a, b):
    return lax.dot_general(a, b, (((1,), (1,)), ((), ())), preferred_element_type=jnp.float32)


def unit_rows(block):
    whole = block.astype(jnp.float32)
    length = jnp.sqrt(jnp.sum(whole * whole, axis=1, keepdims=True) + 1e-06)
    return (whole / length).astype(jnp.bfloat16)


def unit_kernel(x_ref, o_ref):
    o_ref[...] = unit_rows(x_ref[...])


def join_kernel(a_ref, b_ref, o_ref):
    rows = a_ref.shape[0]
    o_ref[:rows] = a_ref[...]
    o_ref[rows:] = b_ref[...]


def store(ref, top, total, start=0):
    columns = pl.ds(start, top.shape[1])
    ref[:SUB, columns] = top
    ref[SUB:, columns] = total


def split_queries(pair, direct, relayed, corner, corner_twin):
    rows = corner.shape[0]
    keep = jnp.concatenate([pair[:rows], direct[...], corner[...]], axis=0)
    give = jnp.concatenate([pair[rows:], relayed[...], corner_twin[...]], axis=0)
    return keep, give


def home_kernel(diagonal, pair, *refs):
    *others, ref = refs
    rows = pair.shape[0] // 2
    first = pair[:rows] if diagonal else pair[rows:]
    table = dots(pair[:rows], jnp.concatenate([first] + [o[...] for o in others], axis=0))
    if diagonal:
        line = lax.broadcasted_iota(jnp.int32, table.shape, 0)
        column = lax.broadcasted_iota(jnp.int32, table.shape, 1)
        table = jnp.where(line == column, -2.0, table)
    best, count = column_lists(table)
    for i in range(TOPK):
        ref[i * SUB : (i + 1) * SUB] = best[i]
    ref[TOPK * SUB :] = count


def score_kernel(n_shift, got, *refs):
    queries, states = refs[:5], refs[5:7]
    pairs = refs[7 : 7 + 2 * n_shift]
    keep_ref, give_ref = refs[7 + 2 * n_shift : 9 + 2 * n_shift]
    back_refs = refs[9 + 2 * n_shift :]
    first = lax.axis_index("rep") % 2 == 0
    key = [jnp.where(first, a[...], b[...]) for a, b in zip(pairs[::2], pairs[1::2])]
    live = got()
    keep, give = split_queries(*queries)
    down = [(dots(keep, k), dots(give, k)) for k in key]
    ahead = [d[0].T for d in down]
    for k in range(n_shift):
        table = jnp.concatenate(down[k], axis=0)
        store(back_refs[k], *fold_sublanes(*column_lists(table)))
    for query, state, ref in ((keep, states[0], keep_ref), (give, states[1], give_ref)):
        best = [state[i * SUB : (i + 1) * SUB] for i in range(TOPK)]
        count = state[TOPK * SUB :]
        tables, ahead = ahead, [d[1].T for d in down] if query is keep else None
        for k in range(n_shift):
            more, more_count = column_lists(tables[k])
            best = merge(best, [jnp.where(live[k], m, LOW) for m in more])
            count = count + jnp.where(live[k], more_count, 0.0)
        store(ref, *fold_sublanes(best, count))


def lists_of(packed):
    shape = (SUB, packed.shape[1])
    row = lambda i: jnp.broadcast_to(packed[i : i + 1], shape)
    return [row(i) for i in range(TOPK)], packed[SUB:]


def stacked(best):
    place = lax.broadcasted_iota(jnp.int32, best[0].shape, 0)
    top = best[0]
    for i in range(1, TOPK):
        top = jnp.where(place == i, best[i], top)
    return top


def pair_kernel(keep_ref, got_ref, own_ref, direct_ref, corner_ref):
    rows = own_ref.shape[1]
    best, count = lists_of(keep_ref[...])
    more, more_count = lists_of(got_ref[...])
    top, total = stacked(merge(best, more)), count + more_count
    store(own_ref, top[:, :rows], total[:, :rows])
    store(direct_ref, top[:, rows : 3 * rows], total[:, rows : 3 * rows])
    store(corner_ref, top[:, 3 * rows :], total[:, 3 * rows :])


def last_kernel(n_shift, gave, own, corner, direct, relayed, *refs):
    mine, theirs = refs[:n_shift], refs[n_shift : 2 * n_shift]
    near_ref, dup_ref = refs[2 * n_shift :]
    rows = own.shape[1]
    found = [lists_of(own[...]), lists_of(corner[...])]
    found += [lists_of(direct[:, :rows]), lists_of(relayed[:, rows:])]
    parts = [m[:, :rows] for m in mine] + [t[:, rows:] for t in theirs]
    for flag, part in zip(gave(False) + gave(True), parts):
        best, count = lists_of(part)
        found.append(([jnp.where(flag, b, LOW) for b in best], jnp.where(flag, count, 0.0)))
    while len(found) > 1:
        paired = [
            (merge(found[i][0], found[i + 1][0]), found[i][1] + found[i + 1][1])
            for i in range(0, len(found) - 1, 2)
        ]
        found = paired + found[len(found) - len(found) % 2 :]
    best, count = found[0]
    near_ref[...] = stacked(best)
    dup_ref[...] = count[:1]


VMEM = pl.BlockSpec(memory_space=pltpu.VMEM)


def call(kernel, args, shapes, keep=True):
    args = [pltpu.with_memory_space_constraint(a, pltpu.VMEM) for a in args]
    return pl.pallas_call(
        kernel,
        out_shape=[(pltpu.VMEM if keep else jax.ShapeDtypeStruct)(*s) for s in shapes],
        in_specs=[VMEM] * len(args),
        out_specs=[VMEM] * len(shapes),
        compiler_params=pltpu.CompilerParams(vmem_limit_bytes=GRANT),
    )(*args)


def body(blocks, reps, embeddings):
    rows, width = embeddings.shape
    deep, wide = blocks // 2, reps // 2
    half = deep // 2
    n_shift = (half + 1) // 2
    f32, bf16 = jnp.float32, jnp.bfloat16

    def flat(z, y, x, c):
        return ((z * 2 + y) * wide + x) * 2 + c

    places = [
        (z, y, x, c) for z in range(deep) for y in range(2) for x in range(wide) for c in range(2)
    ]

    def moved(value, to, reverse=False, cores=(0, 1)):
        perm = [
            (flat(*p), flat(*to(*p))) for p in places if p[3] in cores and to(*p) is not None
        ]
        return lax.ppermute(value, AXES, [(b, a) for a, b in perm] if reverse else perm)

    def swap(z, y, x, c):
        return z, y, x, 1 - c

    def side(z, y, x, c):
        return (z, y, (x + 1) % wide, c) if c == 0 else (z, 1 - y, x, c)

    def corner(z, y, x, c):
        return z, 1 - y, (x + 1) % wide, c

    def shift(j):
        def to(z, y, x, c):
            k = 2 * j + 2 - c
            if k > half:
                return None
            if 2 * k == deep:
                if z < half:
                    return (z + half, y, x, c) if z % 2 == 0 else None
                return (z - half, y, x, c) if (z - half) % 2 == 1 else None
            return (z + k) % deep, y, x, c

        return to

    def flags(other, pick):
        depth = lax.axis_index("blk") // 2
        core = lax.axis_index("rep") % 2
        core = 1 - core if other else core
        sends = jnp.where(depth < half, depth % 2 == 0, (depth - half) % 2 == 1)
        out = []
        for j in range(n_shift):
            k = 2 * j + 2 - core
            whole = 2 * k != deep
            out.append((k <= half) & (whole | (sends == pick)))
        return out

    def gave(other):
        return flags(other, True)

    def got():
        return flags(False, False)

    (unit,) = call(unit_kernel, [embeddings], [((rows, width), bf16)])
    twin = moved(unit, swap)
    corner_rows = moved(unit, corner)
    (pair,) = call(join_kernel, [unit, twin], [((2 * rows, width), bf16)])
    keys = []
    for j in range(n_shift):
        keys += [moved(pair, shift(j), cores=(c,)) for c in range(2)]
    direct = moved(pair, side)
    corner_twin = moved(corner_rows, swap)
    relayed = moved(direct, swap)
    queries = [pair, direct, relayed, corner_rows, corner_twin]

    state = (((TOPK + 1) * SUB, 4 * rows), f32)
    states = call(functools.partial(home_kernel, True), [pair, direct, corner_rows], [state])
    states += call(functools.partial(home_kernel, False), [pair, relayed, corner_twin], [state])
    lists = lambda n: ((PACK, n * rows), f32)
    keep, give, *away = call(
        functools.partial(score_kernel, n_shift, got),
        queries + list(states) + keys,
        [lists(4), lists(4)] + [lists(2)] * n_shift,
    )
    given = moved(give, swap)
    mine = [moved(a, shift(j), reverse=True) for j, a in enumerate(away)]
    own, sides, corners = call(pair_kernel, [keep, given], [lists(1), lists(2), lists(1)])
    direct = moved(sides, side, reverse=True)
    corners = moved(corners, corner, reverse=True)
    theirs = [moved(m, swap) for m in mine]
    relayed = moved(direct, swap)
    near, dup = call(
        functools.partial(last_kernel, n_shift, gave),
        [own, corners, direct, relayed] + mine + theirs,
        [((TOPK, rows), f32), ((1, rows), f32)],
        keep=False,
    )
    return near.T, dup.reshape(rows)


def solution(mesh):
    placed = (P(AXES, None),)

    def layer(embeddings):
        return body(mesh.shape["blk"], mesh.shape["rep"], embeddings)

    return jax.shard_map(
        layer,
        mesh=mesh,
        in_specs=placed,
        out_specs=(P(AXES, None), P(AXES)),
        check_vma=False,
    )
```

```python
import functools
import math

import jax
import jax.numpy as jnp
from jax import lax
from jax.experimental import pallas as pl
from jax.experimental.pallas import tpu as pltpu
from jax.sharding import PartitionSpec as P


TOPK = 8
SUB = 8
PACK = 16
LOW = -4.0
decision_bound = 0.5
sigmoid_sharpness = 0.05
GRANT = 32 * 2**20
AXES = ("blk", "rep")

SOFT_SLOPE = 1.0 / (sigmoid_sharpness * math.log(2.0))
SOFT_BASE = decision_bound * SOFT_SLOPE


SORT8 = (
    (0, 1), (2, 3), (4, 5), (6, 7),
    (0, 2), (1, 3), (4, 6), (5, 7),
    (1, 2), (5, 6), (0, 4), (3, 7),
    (1, 5), (2, 6),
    (1, 4), (3, 6),
    (2, 4), (3, 5),
    (3, 4),
)
BITONIC8 = (
    (0, 4), (1, 5), (2, 6), (3, 7),
    (0, 2), (1, 3), (4, 6), (5, 7),
    (0, 1), (2, 3), (4, 5), (6, 7),
)


def network(values, pairs):
    values = list(values)
    for low, high in pairs:
        a, b = values[low], values[high]
        values[low], values[high] = jnp.maximum(a, b), jnp.minimum(a, b)
    return values


def merge(a, b):
    return network([jnp.maximum(a[i], b[TOPK - 1 - i]) for i in range(TOPK)], BITONIC8)


def soft(table):
    return 1.0 / (1.0 + jnp.exp2(SOFT_BASE - SOFT_SLOPE * table))


def column_lists(table):
    tiles = [table[i : i + SUB] for i in range(0, table.shape[0], SUB)]
    best = None
    for i in range(0, len(tiles), TOPK):
        group = tiles[i : i + TOPK]
        group += [jnp.full_like(tiles[0], LOW)] * (TOPK - len(group))
        group = network(group, SORT8)
        best = group if best is None else merge(best, group)
    count = functools.reduce(jnp.add, [soft(t) for t in tiles])
    return best, count


def fold_sublanes(best, count):
    for step in (4, 2, 1):
        best = merge(best, [pltpu.roll(b, step, 0) for b in best])
        count = count + pltpu.roll(count, step, 0)
    place = lax.broadcasted_iota(jnp.int32, best[0].shape, 0)
    top = best[0]
    for i in range(1, TOPK):
        top = jnp.where(place == i, best[i], top)
    return top, count


def dots(a, b):
    return lax.dot_general(a, b, (((1,), (1,)), ((), ())), preferred_element_type=jnp.float32)


def unit_rows(block):
    whole = block.astype(jnp.float32)
    length = jnp.sqrt(jnp.sum(whole * whole, axis=1, keepdims=True) + 1e-06)
    return (whole / length).astype(jnp.bfloat16)


def unit_kernel(x_ref, o_ref):
    o_ref[...] = unit_rows(x_ref[...])


def join_kernel(a_ref, b_ref, o_ref):
    rows = a_ref.shape[0]
    o_ref[:rows] = a_ref[...]
    o_ref[rows:] = b_ref[...]


def store(ref, top, total, start=0):
    columns = pl.ds(start, top.shape[1])
    ref[:SUB, columns] = top
    ref[SUB:, columns] = total


def split_queries(pair, direct, relayed, corner, corner_twin):
    rows = corner.shape[0]
    keep = jnp.concatenate([pair[:rows], direct[...], corner[...]], axis=0)
    give = jnp.concatenate([pair[rows:], relayed[...], corner_twin[...]], axis=0)
    return keep, give


def home_kernel(diagonal, pair, *refs):
    *others, ref = refs
    rows = pair.shape[0] // 2
    first = pair[:rows] if diagonal else pair[rows:]
    table = dots(pair[:rows], jnp.concatenate([first] + [o[...] for o in others], axis=0))
    if diagonal:
        line = lax.broadcasted_iota(jnp.int32, table.shape, 0)
        column = lax.broadcasted_iota(jnp.int32, table.shape, 1)
        table = jnp.where(line == column, -2.0, table)
    best, count = column_lists(table)
    for i in range(TOPK):
        ref[i * SUB : (i + 1) * SUB] = best[i]
    ref[TOPK * SUB :] = count


def score_kernel(n_shift, got, *refs):
    queries, states = refs[:5], refs[5:7]
    keys = refs[7 : 7 + n_shift]
    keep_ref, give_ref = refs[7 + n_shift : 9 + n_shift]
    back_refs = refs[9 + n_shift :]
    live = got()
    keep, give = split_queries(*queries)
    key = [k[...] for k in keys]
    down = [(dots(keep, k), dots(give, k)) for k in key]
    ahead = [d[0].T for d in down]
    for k in range(n_shift):
        table = jnp.concatenate(down[k], axis=0)
        store(back_refs[k], *fold_sublanes(*column_lists(table)))
    for query, state, ref in ((keep, states[0], keep_ref), (give, states[1], give_ref)):
        best = [state[i * SUB : (i + 1) * SUB] for i in range(TOPK)]
        count = state[TOPK * SUB :]
        tables, ahead = ahead, [d[1].T for d in down] if query is keep else None
        for k in range(n_shift):
            more, more_count = column_lists(tables[k])
            best = merge(best, [jnp.where(live[k], m, LOW) for m in more])
            count = count + jnp.where(live[k], more_count, 0.0)
        store(ref, *fold_sublanes(best, count))


def lists_of(packed):
    shape = (SUB, packed.shape[1])
    row = lambda i: jnp.broadcast_to(packed[i : i + 1], shape)
    return [row(i) for i in range(TOPK)], packed[SUB:]


def stacked(best):
    place = lax.broadcasted_iota(jnp.int32, best[0].shape, 0)
    top = best[0]
    for i in range(1, TOPK):
        top = jnp.where(place == i, best[i], top)
    return top


def pair_kernel(keep_ref, got_ref, own_ref, direct_ref, corner_ref):
    rows = own_ref.shape[1]
    best, count = lists_of(keep_ref[...])
    more, more_count = lists_of(got_ref[...])
    top, total = stacked(merge(best, more)), count + more_count
    store(own_ref, top[:, :rows], total[:, :rows])
    store(direct_ref, top[:, rows : 3 * rows], total[:, rows : 3 * rows])
    store(corner_ref, top[:, 3 * rows :], total[:, 3 * rows :])


def last_kernel(n_shift, gave, own, corner, direct, relayed, *refs):
    mine, theirs = refs[:n_shift], refs[n_shift : 2 * n_shift]
    near_ref, dup_ref = refs[2 * n_shift :]
    rows = own.shape[1]
    found = [lists_of(own[...]), lists_of(corner[...])]
    found += [lists_of(direct[:, :rows]), lists_of(relayed[:, rows:])]
    parts = [m[:, :rows] for m in mine] + [t[:, rows:] for t in theirs]
    for flag, part in zip(gave(False) + gave(True), parts):
        best, count = lists_of(part)
        found.append(([jnp.where(flag, b, LOW) for b in best], jnp.where(flag, count, 0.0)))
    while len(found) > 1:
        paired = [
            (merge(found[i][0], found[i + 1][0]), found[i][1] + found[i + 1][1])
            for i in range(0, len(found) - 1, 2)
        ]
        found = paired + found[len(found) - len(found) % 2 :]
    best, count = found[0]
    near_ref[...] = stacked(best)
    dup_ref[...] = count[:1]


VMEM = pl.BlockSpec(memory_space=pltpu.VMEM)


def call(kernel, args, shapes, keep=True):
    args = [pltpu.with_memory_space_constraint(a, pltpu.VMEM) for a in args]
    return pl.pallas_call(
        kernel,
        out_shape=[(pltpu.VMEM if keep else jax.ShapeDtypeStruct)(*s) for s in shapes],
        in_specs=[VMEM] * len(args),
        out_specs=[VMEM] * len(shapes),
        compiler_params=pltpu.CompilerParams(vmem_limit_bytes=GRANT),
    )(*args)


def body(blocks, reps, embeddings):
    rows, width = embeddings.shape
    deep, wide = blocks // 2, reps // 2
    half = deep // 2
    n_shift = (half + 1) // 2
    f32, bf16 = jnp.float32, jnp.bfloat16

    def flat(z, y, x, c):
        return ((z * 2 + y) * wide + x) * 2 + c

    places = [
        (z, y, x, c) for z in range(deep) for y in range(2) for x in range(wide) for c in range(2)
    ]

    def moved(value, to, reverse=False):
        perm = [(flat(*p), flat(*to(*p))) for p in places if to(*p) is not None]
        return lax.ppermute(value, AXES, [(b, a) for a, b in perm] if reverse else perm)

    def swap(z, y, x, c):
        return z, y, x, 1 - c

    def side(z, y, x, c):
        return (z, y, (x + 1) % wide, c) if c == 0 else (z, 1 - y, x, c)

    def corner(z, y, x, c):
        return z, 1 - y, (x + 1) % wide, c

    def shift(j):
        def to(z, y, x, c):
            k = 2 * j + 2 - c
            if k > half:
                return None
            if 2 * k == deep:
                if z < half:
                    return (z + half, y, x, c) if z % 2 == 0 else None
                return (z - half, y, x, c) if (z - half) % 2 == 1 else None
            return (z + k) % deep, y, x, c

        return to

    def flags(other, pick):
        depth = lax.axis_index("blk") // 2
        core = lax.axis_index("rep") % 2
        core = 1 - core if other else core
        sends = jnp.where(depth < half, depth % 2 == 0, (depth - half) % 2 == 1)
        out = []
        for j in range(n_shift):
            k = 2 * j + 2 - core
            whole = 2 * k != deep
            out.append((k <= half) & (whole | (sends == pick)))
        return out

    def gave(other):
        return flags(other, True)

    def got():
        return flags(False, False)

    (unit,) = call(unit_kernel, [embeddings], [((rows, width), bf16)])
    twin = moved(unit, swap)
    corner_rows = moved(unit, corner)
    (pair,) = call(join_kernel, [unit, twin], [((2 * rows, width), bf16)])
    keys = [moved(pair, shift(j)) for j in range(n_shift)]
    direct = moved(pair, side)
    corner_twin = moved(corner_rows, swap)
    relayed = moved(direct, swap)
    queries = [pair, direct, relayed, corner_rows, corner_twin]

    state = (((TOPK + 1) * SUB, 4 * rows), f32)
    states = call(functools.partial(home_kernel, True), [pair, direct, corner_rows], [state])
    states += call(functools.partial(home_kernel, False), [pair, relayed, corner_twin], [state])
    lists = lambda n: ((PACK, n * rows), f32)
    keep, give, *away = call(
        functools.partial(score_kernel, n_shift, got),
        queries + list(states) + keys,
        [lists(4), lists(4)] + [lists(2)] * n_shift,
    )
    given = moved(give, swap)
    mine = [moved(a, shift(j), reverse=True) for j, a in enumerate(away)]
    own, sides, corners = call(pair_kernel, [keep, given], [lists(1), lists(2), lists(1)])
    direct = moved(sides, side, reverse=True)
    corners = moved(corners, corner, reverse=True)
    theirs = [moved(m, swap) for m in mine]
    relayed = moved(direct, swap)
    near, dup = call(
        functools.partial(last_kernel, n_shift, gave),
        [own, corners, direct, relayed] + mine + theirs,
        [((TOPK, rows), f32), ((1, rows), f32)],
        keep=False,
    )
    return near.T, dup.reshape(rows)


def solution(mesh):
    placed = (P(AXES, None),)

    def layer(embeddings):
        return body(mesh.shape["blk"], mesh.shape["rep"], embeddings)

    return jax.shard_map(
        layer,
        mesh=mesh,
        in_specs=placed,
        out_specs=(P(AXES, None), P(AXES)),
        check_vma=False,
    )
```
